256 devices in a mesh: grp: 8 (over z_lo, x), leaf: 32 (over y, z_hi, core).
Axes of the slice: x: 4, y: 4, z: 8 (z_hi: 4, z_lo: 2; z = z_hi * 2 + z_lo), core: 2. Of those that a mesh axis runs over, the one named last changes fastest.
Arguments:
- snapshots: float32 [1048576, 256], P(('grp', 'leaf')), may hold values from -150 to 150
- sketch: float32 [256, 64], replicated, may hold values from -6 to 6
Outputs:
- recon: bfloat16 [1048576, 256], P(('grp', 'leaf'))
The draws below stay inside these ranges and needn't reach their ends.
All inputs are finite; a program needn't handle non-finite values.
Results may differ from the reference program's by a relative error of at most 0.001.
Values sent between devices are 32-bit elements; how exact they have to be, the bound alone decides.
No kernel may reach another device: no remote copies, remote signals or barrier semaphores. Data moves between devices by JAX's collectives and lax.ppermute only.
A program may use at most 64 MiB of HBM per device.

```python
import math
import jax
import jax.numpy as jnp
from jax import lax

COLS = 256
MODES = 64
ITERS = 1
ROW_DEV = 4096
ROWS = 1048576
N_GRP = 8
N_LEAF = 32


def draw_snapshots(key, part):
    keys = jax.random.split(jax.random.fold_in(key, 7), 6)
    slab_count = ROWS // ROW_DEV
    position = jnp.arange(ROWS, dtype=jnp.float32) / ROWS
    row_scale = jnp.exp(position * math.log(3.0))[:, None] * jnp.exp(jax.random.uniform(keys[0], (ROWS, 1), jnp.float32, 0.0, math.log(2.0)))
    mode_index = jnp.arange(COLS, dtype=jnp.float32)
    basis_key = keys[5]
    decay = math.log(0.3) / MODES
    drop = 6.0
    loadings = jnp.clip(jax.random.normal(keys[2], (ROWS, COLS), jnp.float32), -6.0, 6.0)
    noise_level = 0.04
    col_scale = jnp.exp(jax.random.uniform(keys[1], (1, COLS), jnp.float32, 0.0, math.log(10.0)))
    orthogonal, upper = jnp.linalg.qr(jax.random.normal(basis_key, (COLS, COLS), jnp.float32))
    spectrum = jnp.exp(decay * mode_index) * jnp.where(mode_index < MODES, 1.0, 1.0 / drop)
    jitter = jnp.exp(jax.random.uniform(keys[3], (slab_count, 1, COLS), jnp.float32, -0.5 * math.log(2.0), 0.5 * math.log(2.0)))
    weighted = (loadings.reshape(slab_count, ROW_DEV, COLS) * spectrum[None, None, :] * jitter).reshape(ROWS, COLS)
    field = jnp.dot(weighted, orthogonal.T, precision=jax.lax.Precision.HIGHEST)
    noise = jnp.clip(jax.random.normal(keys[4], (ROWS, COLS), jnp.float32), -6.0, 6.0)
    values = 2.0 * (field + noise_level * noise) * col_scale * row_scale
    return jnp.clip(values, -150.0, 150.0).astype(jnp.float32)


def scatter_about(stream_key, shape, spread, bound, kind=jnp.bfloat16):
    return jnp.clip(spread * jax.random.normal(stream_key, shape, jnp.float32), -bound, bound).astype(kind)


def setup_inputs(seed: int = 0) -> dict:
    streams_of = jax.random.split(jax.random.key(seed), 3)
    snapshots = draw_snapshots(jax.random.fold_in(streams_of[2], 71), 0)
    sketch = scatter_about(streams_of[1], (COLS, MODES), 1.0, 6.0, jnp.float32)
    return {"snapshots": snapshots, "sketch": sketch}


highest_precision = lax.Precision.HIGHEST

def orthonormal(candidate):
    for repeat_index in range(2):
        correlation = jnp.dot(candidate.T, candidate, precision=highest_precision)
        lower_factor = jnp.linalg.cholesky(correlation)
        candidate = jax.scipy.linalg.solve_triangular(lower_factor, candidate.T, lower=True).T
    return candidate

def subspace(gram_sum, sketch):
    mode_basis = orthonormal(jnp.dot(gram_sum, sketch, precision=highest_precision))
    for repeat_index in range(ITERS - 1):
        mode_basis = orthonormal(jnp.dot(gram_sum, mode_basis, precision=highest_precision))
    return mode_basis

def factor(gram_sum, sketch):
    mode_basis = subspace(gram_sum, sketch)
    reduced = jnp.dot(mode_basis.T, jnp.dot(gram_sum, mode_basis, precision=highest_precision), precision=highest_precision)
    reduced = 0.5 * (reduced + reduced.T)
    lower_factor = jnp.linalg.cholesky(reduced)
    return jnp.dot(lower_factor.T, mode_basis.T, precision=highest_precision)

def reference(snapshots, sketch):
    slabs = snapshots.reshape(N_GRP * N_LEAF, ROW_DEV, COLS)

    def slab_factor(slab):
        return factor(jnp.dot(slab.T.astype(jnp.float32), slab.astype(jnp.float32), precision=highest_precision, preferred_element_type=jnp.float32), sketch)
    first_factor = lax.map(slab_factor, slabs).reshape(N_GRP, N_LEAF, MODES, COLS)
    group_gram = jnp.einsum('glmc,glmd->lcd', first_factor, first_factor, precision=highest_precision)
    second_factor = jax.vmap(lambda gram_sum: factor(gram_sum, sketch))(group_gram)
    total_gram = jnp.einsum('lmc,lmd->cd', second_factor, second_factor, precision=highest_precision)
    mode_basis = subspace(total_gram, sketch)
    projector = jnp.dot(mode_basis, mode_basis.T, precision=highest_precision)

    def project(slab):
        return jnp.dot(slab, projector, precision=highest_precision).astype(jnp.bfloat16)
    recon = lax.map(project, slabs)
    return recon.reshape(ROWS, COLS)
```

```python
import jax
import jax.numpy as jnp
from jax import lax
from jax.experimental import pallas as pl
from jax.experimental.pallas import tpu as pltpu
from jax.sharding import PartitionSpec as P

ROWS = 4096
COLS = 256
MODES = 64
TILE = 8
PANELS = MODES // TILE
LANES = 128
STEPS = 8
HIGHEST = lax.Precision.HIGHEST


def dot(a, b):
    return jnp.dot(a, b, precision=HIGHEST, preferred_element_type=jnp.float32)


def dot_nt(a, b):
    return lax.dot_general(
        a, b, (((1,), (1,)), ((), ())), precision=HIGHEST, preferred_element_type=jnp.float32
    )


def dot_tn(a, b):
    return lax.dot_general(
        a, b, (((0,), (0,)), ((), ())), precision=HIGHEST, preferred_element_type=jnp.float32
    )


def gram_of_rows(a):
    high, mid, low = split3(a)
    half = jnp.bfloat16(0.5)
    dims = (((0,), (0,)), ((), ()))
    upper = lax.dot_general(high, high * half, dims, preferred_element_type=jnp.float32)
    upper += lax.dot_general(high, mid, dims, preferred_element_type=jnp.float32)
    upper += lax.dot_general(high, low, dims, preferred_element_type=jnp.float32)
    upper += lax.dot_general(mid, mid * half, dims, preferred_element_type=jnp.float32)
    return upper


def split3(a):
    high = a.astype(jnp.bfloat16)
    rest = a - high.astype(jnp.float32)
    mid = rest.astype(jnp.bfloat16)
    low = (rest - mid.astype(jnp.float32)).astype(jnp.bfloat16)
    return high, mid, low


def split2(a):
    high = a.astype(jnp.bfloat16)
    return high, (a - high.astype(jnp.float32)).astype(jnp.bfloat16)


def lane_splat(tile, lane):
    return jnp.broadcast_to(tile[:, lane : lane + 1], (TILE, LANES))


def row_splat(tile, row):
    return jnp.broadcast_to(tile[row : row + 1, :], tile.shape)


def eliminate(square, others):
    sublane = lax.broadcasted_iota(jnp.int32, (TILE, LANES), 0)
    rows = [
        [m[TILE * i : TILE * (i + 1), :] for m in (square, *others)] for i in range(PANELS)
    ]
    diag = [lane_splat(rows[0][0], j) for j in range(TILE)]
    for t in range(PANELS):
        base = TILE * t
        below = {
            i: [lane_splat(rows[i][0], base + j) for j in range(TILE)]
            for i in range(t + 1, PANELS)
        }
        ahead = (
            [lane_splat(rows[t + 1][0], base + TILE + l) for l in range(TILE)]
            if t + 1 < PANELS
            else None
        )
        pivots = None
        for j in range(TILE):
            pivot = row_splat(diag[j], j)
            inverse = 1.0 / pivot
            pivots = pivot if pivots is None else jnp.where(sublane == j, pivot, pivots)
            pivot_rows = [row_splat(part, j) for part in rows[t]]
            column = {l: row_splat(diag[l], j) for l in range(j + 1, TILE)}
            if j + 1 < TILE:
                factor = jnp.where(sublane > j, diag[j] * inverse, 0.0)
                for l in range(j + 1, TILE):
                    diag[l] = diag[l] - factor * column[l]
                rows[t] = [part - factor * row for part, row in zip(rows[t], pivot_rows)]
            for i in range(t + 1, PANELS):
                factor = below[i][j] * inverse
                if i == t + 1:
                    for l in range(TILE):
                        ahead[l] = ahead[l] - factor * row_splat(below[i][j], l)
                for l in range(j + 1, TILE):
                    below[i][l] = below[i][l] - factor * column[l]
                rows[i] = [part - factor * row for part, row in zip(rows[i], pivot_rows)]
        scale = lax.rsqrt(pivots)
        rows[t] = [part * scale for part in rows[t]]
        diag = ahead
    count = 1 + len(others)
    return [jnp.concatenate([rows[i][k] for i in range(PANELS)], axis=0) for k in range(count)]


def halves(a):
    return [a[:, :LANES], a[:, LANES:]]


def wide(a):
    return jnp.concatenate([a, jnp.zeros_like(a)], axis=0)


def identity_right():
    row = lax.broadcasted_iota(jnp.int32, (MODES, LANES), 0)
    lane = lax.broadcasted_iota(jnp.int32, (MODES, LANES), 1)
    return jnp.where(lane == row + MODES, 1.0, 0.0).astype(jnp.float32)


def first_pass(sample):
    _, *parts = eliminate(dot_nt(sample, wide(sample)), halves(sample))
    return jnp.concatenate(parts, axis=1)


def second_pass(rough):
    square, *parts = eliminate(dot_nt(rough, wide(rough)) + identity_right(), halves(rough))
    return square[:, MODES:], jnp.concatenate(parts, axis=1)


def leaf_kernel(snap_ref, sketch_ref, out_ref, gram_ref):
    step = pl.program_id(0)
    part = gram_of_rows(snap_ref[...])

    @pl.when(step == 0)
    def _():
        gram_ref[...] = part

    @pl.when(step > 0)
    def _():
        gram_ref[...] += part

    @pl.when(step == STEPS - 1)
    def _():
        half = gram_ref[...]
        gram = half + half.T
        rough = first_pass(dot(sketch_ref[...], gram))
        inner = dot_nt(dot(rough, gram), wide(rough))
        inverse, basis = second_pass(rough)
        (inner_factor,) = eliminate(inner, [])
        out_ref[...] = dot(dot_nt(inner_factor[:, :MODES], inverse), basis)


def first_factor(snapshots, sketch_rows):
    return pl.pallas_call(
        leaf_kernel,
        grid=(STEPS,),
        out_shape=jax.ShapeDtypeStruct((MODES, COLS), jnp.float32),
        in_specs=[
            pl.BlockSpec((ROWS // STEPS, COLS), lambda i: (i, 0)),
            pl.BlockSpec((MODES, COLS), lambda i: (0, 0)),
        ],
        out_specs=pl.BlockSpec((MODES, COLS), lambda i: (0, 0)),
        scratch_shapes=[pltpu.VMEM((COLS, COLS), jnp.float32)],
        name="leaf_factor",
    )(snapshots, sketch_rows)


def group_kernel(factors_ref, sketch_ref, out_ref):
    half = gram_of_rows(factors_ref[...])
    gram = half + half.T
    sketch = sketch_ref[...]
    rough = first_pass(dot(sketch, gram))
    inner = dot_nt(dot(rough, gram), rough)
    overlap = dot_nt(sketch, rough)
    inverse, basis = second_pass(rough)
    mixed = dot(dot_nt(overlap, inverse), dot(inverse, inner))
    out_ref[...] = dot(dot_nt(mixed, inverse), basis)


def group_sample(factors, sketch_rows):
    return pl.pallas_call(
        group_kernel,
        out_shape=jax.ShapeDtypeStruct((MODES, COLS), jnp.float32),
        in_specs=[pl.BlockSpec(memory_space=pltpu.VMEM)] * 2,
        out_specs=pl.BlockSpec(memory_space=pltpu.VMEM),
        name="group_sample",
    )(factors, sketch_rows)


def project_kernel(snap_ref, sample_ref, out_ref, snap_vmem, out_vmem, in_sem, out_sem):
    block = ROWS // STEPS
    loads = [
        pltpu.make_async_copy(
            snap_ref.at[pl.ds(k * block, block)], snap_vmem.at[pl.ds(k * block, block)], in_sem.at[k]
        )
        for k in range(STEPS)
    ]
    for load in loads:
        load.start()
    _, basis = second_pass(first_pass(sample_ref[...]))
    high, low = split2(dot_tn(basis, basis))
    stores = []
    for k in range(STEPS):
        loads[k].wait()
        rows = pl.ds(k * block, block)
        snap_high, snap_low = split2(snap_vmem[rows, :])
        value = jnp.dot(snap_high, high, preferred_element_type=jnp.float32)
        value += jnp.dot(snap_low, high, preferred_element_type=jnp.float32)
        value += jnp.dot(snap_high, low, preferred_element_type=jnp.float32)
        out_vmem[rows, :] = value.astype(jnp.bfloat16)
        store = pltpu.make_async_copy(out_vmem.at[rows], out_ref.at[rows], out_sem.at[k])
        store.start()
        stores.append(store)
    for store in stores:
        store.wait()


def project(snapshots, sample):
    return pl.pallas_call(
        project_kernel,
        out_shape=jax.ShapeDtypeStruct((ROWS, COLS), jnp.bfloat16),
        in_specs=[
            pl.BlockSpec(memory_space=pl.ANY),
            pl.BlockSpec(memory_space=pltpu.VMEM),
        ],
        out_specs=pl.BlockSpec(memory_space=pl.ANY),
        scratch_shapes=[
            pltpu.VMEM((ROWS, COLS), jnp.float32),
            pltpu.VMEM((ROWS, COLS), jnp.bfloat16),
            pltpu.SemaphoreType.DMA((STEPS,)),
            pltpu.SemaphoreType.DMA((STEPS,)),
        ],
        name="project",
    )(snapshots, sample)


def to_all(array, axis):
    copies = jnp.broadcast_to(array, (lax.axis_size(axis), *array.shape))
    return lax.all_to_all(copies, axis, split_axis=0, concat_axis=0, tiled=True)


def local(snapshots, sketch):
    sketch_rows = sketch.T
    factors = to_all(first_factor(snapshots, sketch_rows), "grp")
    sample = group_sample(factors.reshape(-1, COLS), sketch_rows)
    share = MODES // lax.axis_size("grp")
    slot = lax.axis_index("grp") * share
    mine = lax.dynamic_slice_in_dim(sample, slot, share, 0)
    summed = jnp.sum(to_all(mine, "leaf"), axis=0)
    total = to_all(summed, "grp").reshape(MODES, COLS)
    return project(snapshots, total)


def solution(mesh):
    return jax.shard_map(
        local,
        mesh=mesh,
        in_specs=(P(("grp", "leaf"), None), P()),
        out_specs=P(("grp", "leaf"), None),
        check_vma=False,
    )
```

```python
import jax
import jax.numpy as jnp
from jax import lax
from jax.experimental import pallas as pl
from jax.experimental.pallas import tpu as pltpu
from jax.sharding import PartitionSpec as P

ROWS = 4096
COLS = 256
MODES = 64
TILE = 8
PANELS = MODES // TILE
LANES = 128
STEPS = 8
MIB = 2**20
HIGHEST = lax.Precision.HIGHEST


def dot(a, b):
    return jnp.dot(a, b, precision=HIGHEST, preferred_element_type=jnp.float32)


def dot_nt(a, b):
    return lax.dot_general(
        a, b, (((1,), (1,)), ((), ())), precision=HIGHEST, preferred_element_type=jnp.float32
    )


def dot_tn(a, b):
    return lax.dot_general(
        a, b, (((0,), (0,)), ((), ())), precision=HIGHEST, preferred_element_type=jnp.float32
    )


def gram_of_rows(a):
    high, mid, low = split3(a)
    half = jnp.bfloat16(0.5)
    dims = (((0,), (0,)), ((), ()))
    upper = lax.dot_general(high, high * half, dims, preferred_element_type=jnp.float32)
    upper += lax.dot_general(high, mid, dims, preferred_element_type=jnp.float32)
    upper += lax.dot_general(high, low, dims, preferred_element_type=jnp.float32)
    upper += lax.dot_general(mid, mid * half, dims, preferred_element_type=jnp.float32)
    return upper


def split3(a):
    high = a.astype(jnp.bfloat16)
    rest = a - high.astype(jnp.float32)
    mid = rest.astype(jnp.bfloat16)
    low = (rest - mid.astype(jnp.float32)).astype(jnp.bfloat16)
    return high, mid, low


def split2(a):
    high = a.astype(jnp.bfloat16)
    return high, (a - high.astype(jnp.float32)).astype(jnp.bfloat16)


def lane_splat(tile, lane):
    return jnp.broadcast_to(tile[:, lane : lane + 1], (TILE, LANES))


def row_splat(tile, row):
    return jnp.broadcast_to(tile[row : row + 1, :], tile.shape)


def eliminate(square, others):
    sublane = lax.broadcasted_iota(jnp.int32, (TILE, LANES), 0)
    rows = [
        [m[TILE * i : TILE * (i + 1), :] for m in (square, *others)] for i in range(PANELS)
    ]
    diag = [lane_splat(rows[0][0], j) for j in range(TILE)]
    for t in range(PANELS):
        base = TILE * t
        below = {
            i: [lane_splat(rows[i][0], base + j) for j in range(TILE)]
            for i in range(t + 1, PANELS)
        }
        ahead = (
            [lane_splat(rows[t + 1][0], base + TILE + l) for l in range(TILE)]
            if t + 1 < PANELS
            else None
        )
        pivots = None
        for j in range(TILE):
            pivot = row_splat(diag[j], j)
            inverse = 1.0 / pivot
            pivots = pivot if pivots is None else jnp.where(sublane == j, pivot, pivots)
            pivot_rows = [row_splat(part, j) for part in rows[t]]
            column = {l: row_splat(diag[l], j) for l in range(j + 1, TILE)}
            if j + 1 < TILE:
                factor = jnp.where(sublane > j, diag[j] * inverse, 0.0)
                for l in range(j + 1, TILE):
                    diag[l] = diag[l] - factor * column[l]
                rows[t] = [part - factor * row for part, row in zip(rows[t], pivot_rows)]
            for i in range(t + 1, PANELS):
                factor = below[i][j] * inverse
                if i == t + 1:
                    for l in range(TILE):
                        ahead[l] = ahead[l] - factor * row_splat(below[i][j], l)
                for l in range(j + 1, TILE):
                    below[i][l] = below[i][l] - factor * column[l]
                rows[i] = [part - factor * row for part, row in zip(rows[i], pivot_rows)]
        scale = lax.rsqrt(pivots)
        rows[t] = [part * scale for part in rows[t]]
        diag = ahead
    count = 1 + len(others)
    return [jnp.concatenate([rows[i][k] for i in range(PANELS)], axis=0) for k in range(count)]


def halves(a):
    return [a[:, :LANES], a[:, LANES:]]


def wide(a):
    return jnp.concatenate([a, jnp.zeros_like(a)], axis=0)


def identity_right():
    row = lax.broadcasted_iota(jnp.int32, (MODES, LANES), 0)
    lane = lax.broadcasted_iota(jnp.int32, (MODES, LANES), 1)
    return jnp.where(lane == row + MODES, 1.0, 0.0).astype(jnp.float32)


def first_pass(sample):
    _, *parts = eliminate(dot_nt(sample, wide(sample)), halves(sample))
    return jnp.concatenate(parts, axis=1)


def second_pass(rough):
    square, *parts = eliminate(dot_nt(rough, wide(rough)) + identity_right(), halves(rough))
    return square[:, MODES:], jnp.concatenate(parts, axis=1)


def chunk_loads(snap_ref, snap_vmem, sem):
    block = ROWS // STEPS

    def load(k):
        rows = pl.ds(pl.multiple_of(k * block, block), block)
        return pltpu.make_async_copy(snap_ref.at[rows], snap_vmem.at[rows], sem.at[k])

    for k in range(STEPS):
        load(k).start()
    return load


def leaf_kernel(snap_ref, sketch_ref, out_ref, snap_vmem, gram_ref, sem):
    block = ROWS // STEPS
    load = chunk_loads(snap_ref, snap_vmem, sem)
    gram_ref[...] = jnp.zeros_like(gram_ref)

    @pl.loop(0, STEPS)
    def _(k):
        load(k).wait()
        gram_ref[...] += gram_of_rows(snap_vmem[pl.ds(pl.multiple_of(k * block, block), block), :])

    half = gram_ref[...]
    gram = half + half.T
    rough = first_pass(dot(sketch_ref[...], gram))
    inner = dot_nt(dot(rough, gram), wide(rough))
    inverse, basis = second_pass(rough)
    (inner_factor,) = eliminate(inner, [])
    factor = dot(dot_nt(inner_factor[:, :MODES], inverse), basis)
    for copy in range(out_ref.shape[0]):
        out_ref[copy] = factor


def first_factor(snapshots, sketch_rows, copies):
    return pl.pallas_call(
        leaf_kernel,
        out_shape=jax.ShapeDtypeStruct((copies, MODES, COLS), jnp.float32),
        in_specs=[
            pl.BlockSpec(memory_space=pltpu.HBM),
            pl.BlockSpec(memory_space=pltpu.VMEM),
        ],
        out_specs=pl.BlockSpec(memory_space=pltpu.VMEM),
        scratch_shapes=[
            pltpu.VMEM((ROWS, COLS), jnp.float32),
            pltpu.VMEM((COLS, COLS), jnp.float32),
            pltpu.SemaphoreType.DMA((STEPS,)),
        ],
        compiler_params=pltpu.CompilerParams(vmem_limit_bytes=51 * MIB),
        name="leaf_factor",
    )(snapshots, sketch_rows)


def group_kernel(factors_ref, sketch_ref, out_ref):
    half = gram_of_rows(factors_ref[...].reshape(-1, COLS))
    gram = half + half.T
    rough = first_pass(dot(sketch_ref[...], gram))
    inner = dot_nt(dot(rough, gram), rough)
    share = out_ref.shape[0]
    slot = pl.multiple_of(lax.axis_index("grp") * share, share)
    overlap = dot_nt(sketch_ref[pl.ds(slot, share), :], rough)
    inverse, basis = second_pass(rough)
    mixed = dot(dot_nt(overlap, inverse), dot(inverse, inner))
    out_ref[...] = dot(dot_nt(mixed, inverse), basis)


def group_sample(factors, sketch_rows):
    share = MODES // factors.shape[0]
    return pl.pallas_call(
        group_kernel,
        out_shape=jax.ShapeDtypeStruct((share, COLS), jnp.float32),
        in_specs=[pl.BlockSpec(memory_space=pltpu.VMEM)] * 2,
        out_specs=pl.BlockSpec(memory_space=pltpu.VMEM),
        compiler_params=pltpu.CompilerParams(vmem_limit_bytes=16 * MIB),
        name="group_sample",
    )(factors, sketch_rows)


def project_kernel(snap_ref, sample_ref, out_ref, snap_vmem, out_vmem, in_sem, out_sem):
    block = ROWS // STEPS
    load = chunk_loads(snap_ref, snap_vmem, in_sem)
    _, basis = second_pass(first_pass(sample_ref[...]))
    high, low = split2(dot_tn(basis, basis))

    def store(k):
        rows = pl.ds(pl.multiple_of(k * block, block), block)
        return pltpu.make_async_copy(out_vmem.at[rows], out_ref.at[rows], out_sem.at[k])

    @pl.loop(0, STEPS)
    def _(k):
        load(k).wait()
        rows = pl.ds(pl.multiple_of(k * block, block), block)
        snap_high, snap_low = split2(snap_vmem[rows, :])
        value = jnp.dot(snap_high, high, preferred_element_type=jnp.float32)
        value += jnp.dot(snap_low, high, preferred_element_type=jnp.float32)
        value += jnp.dot(snap_high, low, preferred_element_type=jnp.float32)
        out_vmem[rows, :] = value.astype(jnp.bfloat16)
        store(k).start()

    @pl.loop(0, STEPS)
    def _(k):
        store(k).wait()


def project(snapshots, sample):
    return pl.pallas_call(
        project_kernel,
        out_shape=jax.ShapeDtypeStruct((ROWS, COLS), jnp.bfloat16),
        in_specs=[
            pl.BlockSpec(memory_space=pltpu.HBM),
            pl.BlockSpec(memory_space=pltpu.VMEM),
        ],
        out_specs=pl.BlockSpec(memory_space=pltpu.HBM),
        scratch_shapes=[
            pltpu.VMEM((ROWS, COLS), jnp.float32),
            pltpu.VMEM((ROWS, COLS), jnp.bfloat16),
            pltpu.SemaphoreType.DMA((STEPS,)),
            pltpu.SemaphoreType.DMA((STEPS,)),
        ],
        compiler_params=pltpu.CompilerParams(vmem_limit_bytes=51 * MIB),
        name="project",
    )(snapshots, sample)


def to_all(copies, axis, groups=None):
    return lax.all_to_all(
        copies, axis, split_axis=0, concat_axis=0, tiled=True, axis_index_groups=groups
    )


def copied(array, count):
    return jnp.broadcast_to(array, (count, *array.shape))


def local(snapshots, sketch):
    sketch_rows = sketch.T
    members, leaves = lax.axis_size("grp"), lax.axis_size("leaf")
    factors = to_all(first_factor(snapshots, sketch_rows, members), "grp")
    mine = group_sample(factors, sketch_rows)
    mine = mine + lax.ppermute(mine, "leaf", [(i, i ^ 1) for i in range(leaves)])
    chips = [list(range(core, leaves, 2)) for core in range(2)]
    summed = jnp.sum(to_all(copied(mine, leaves // 2), "leaf", chips), axis=0)
    total = to_all(copied(summed, members), "grp").reshape(MODES, COLS)
    return project(snapshots, total)


def solution(mesh):
    return jax.shard_map(
        local,
        mesh=mesh,
        in_specs=(P(("grp", "leaf"), None), P()),
        out_specs=P(("grp", "leaf"), None),
        check_vma=False,
    )
```

```python
import jax
import jax.numpy as jnp
from jax import lax
from jax.experimental import pallas as pl
from jax.experimental.pallas import tpu as pltpu
from jax.sharding import PartitionSpec as P

ROWS = 4096
COLS = 256
MODES = 64
TILE = 8
PANELS = MODES // TILE
LANES = 128
STEPS = 8
PAIR = 2
MIB = 2**20


def product(a, b, dims):
    rows = a.shape[0]
    high, mid, low = split3(a)
    b_high, b_mid, b_low = split3(b)
    by_high = partial_product(jnp.concatenate([high, mid, low], axis=0), b_high, dims)
    by_mid = partial_product(jnp.concatenate([high, mid], axis=0), b_mid, dims)
    by_low = partial_product(high, b_low, dims)
    small = by_low + by_high[2 * rows :] + by_mid[rows:]
    return by_high[:rows] + (by_high[rows : 2 * rows] + by_mid[:rows] + small)


def partial_product(a, b, dims):
    return lax.dot_general(a, b, dims, preferred_element_type=jnp.float32)


def dot(a, b):
    return product(a, b, (((1,), (0,)), ((), ())))


def dot_nt(a, b):
    return product(a, b, (((1,), (1,)), ((), ())))


def gram_of_rows(a):
    high, mid, low = split3(a)
    half = jnp.bfloat16(0.5)
    dims = (((0,), (0,)), ((), ()))
    upper = lax.dot_general(high, high * half, dims, preferred_element_type=jnp.float32)
    upper += lax.dot_general(high, mid, dims, preferred_element_type=jnp.float32)
    upper += lax.dot_general(high, low, dims, preferred_element_type=jnp.float32)
    upper += lax.dot_general(mid, mid * half, dims, preferred_element_type=jnp.float32)
    return upper


def split3(a):
    high = a.astype(jnp.bfloat16)
    rest = a - high.astype(jnp.float32)
    mid = rest.astype(jnp.bfloat16)
    low = (rest - mid.astype(jnp.float32)).astype(jnp.bfloat16)
    return high, mid, low


def split2(a):
    high = a.astype(jnp.bfloat16)
    return high, (a - high.astype(jnp.float32)).astype(jnp.bfloat16)


def lane_splat(tile, lane):
    lanes = lax.broadcasted_iota(jnp.int32, (TILE, LANES), 1)
    one = jnp.sum(jnp.where(lanes == lane, tile, 0.0), axis=1, keepdims=True)
    return jnp.broadcast_to(one, (TILE, LANES))


def row_splat(tile, row):
    return jnp.broadcast_to(tile[row : row + 1, :], tile.shape)


def eliminate(square, others):
    sublane = lax.broadcasted_iota(jnp.int32, (TILE, LANES), 0)
    rows = [
        [m[TILE * i : TILE * (i + 1), :] for m in (square, *others)] for i in range(PANELS)
    ]
    diag = [lane_splat(rows[0][0], j) for j in range(TILE)]
    for t in range(PANELS):
        base = TILE * t
        below = {i: [None] * TILE for i in range(t + 1, PANELS)}
        for j in range(TILE):
            for i in range(t + 1, PANELS):
                below[i][j] = lane_splat(rows[i][0], base + j)
        ahead = (
            [lane_splat(rows[t + 1][0], base + TILE + l) for l in range(TILE)]
            if t + 1 < PANELS
            else None
        )
        pivots = None
        for j in range(TILE):
            pivot = row_splat(diag[j], j)
            inverse = 1.0 / pivot
            pivots = pivot if pivots is None else jnp.where(sublane == j, pivot, pivots)
            pivot_rows = [row_splat(part, j) for part in rows[t]]
            column = {l: row_splat(diag[l], j) for l in range(j + 1, TILE)}
            if j + 1 < TILE:
                factor = jnp.where(sublane > j, diag[j] * inverse, 0.0)
                for l in range(j + 1, TILE):
                    diag[l] = diag[l] - factor * column[l]
                rows[t] = [part - factor * row for part, row in zip(rows[t], pivot_rows)]
            for i in range(t + 1, PANELS):
                factor = below[i][j] * inverse
                if i == t + 1:
                    for l in range(TILE):
                        ahead[l] = ahead[l] - factor * row_splat(below[i][j], l)
                for l in range(j + 1, TILE):
                    below[i][l] = below[i][l] - factor * column[l]
                rows[i] = [part - factor * row for part, row in zip(rows[i], pivot_rows)]
        scale = lax.rsqrt(pivots)
        rows[t] = [part * scale for part in rows[t]]
        diag = ahead
    count = 1 + len(others)
    return [jnp.concatenate([rows[i][k] for i in range(PANELS)], axis=0) for k in range(count)]


def halves(a):
    return [a[:, :LANES], a[:, LANES:]]


def wide(a):
    return jnp.concatenate([a, jnp.zeros_like(a)], axis=0)


def identity_right():
    row = lax.broadcasted_iota(jnp.int32, (MODES, LANES), 0)
    lane = lax.broadcasted_iota(jnp.int32, (MODES, LANES), 1)
    return jnp.where(lane == row + MODES, 1.0, 0.0).astype(jnp.float32)


def first_pass(sample):
    _, *parts = eliminate(dot_nt(sample, wide(sample)), halves(sample))
    return jnp.concatenate(parts, axis=1)


def second_pass(rough):
    square, *parts = eliminate(dot_nt(rough, wide(rough)) + identity_right(), halves(rough))
    return square[:, MODES:], jnp.concatenate(parts, axis=1)


def chunk_loads(snap_ref, snap_vmem, sem):
    block = ROWS // STEPS

    def load(k):
        rows = pl.ds(pl.multiple_of(k * block, block), block)
        return pltpu.make_async_copy(snap_ref.at[rows], snap_vmem.at[rows], sem.at[k])

    for k in range(STEPS):
        load(k).start()
    return load


def leaf_kernel(snap_ref, sketch_hbm, out_ref, snap_vmem, sketch_ref, gram_ref, sem, sketch_sem):
    load = chunk_loads(snap_ref, snap_vmem, sem)
    sketch_load = pltpu.make_async_copy(sketch_hbm, sketch_ref, sketch_sem)
    sketch_load.start()
    gram_ref[...] = jnp.zeros_like(gram_ref)

    block = PAIR * ROWS // STEPS

    @pl.loop(0, STEPS // PAIR)
    def _(k):
        for part in range(PAIR):
            load(PAIR * k + part).wait()
        gram_ref[...] += gram_of_rows(snap_vmem[pl.ds(pl.multiple_of(k * block, block), block), :])

    sketch_load.wait()
    half = gram_ref[...]
    gram = half + half.T
    rough = first_pass(dot(sketch_ref[...], gram))
    inner = dot_nt(dot(rough, gram), wide(rough))
    inverse, basis = second_pass(rough)
    (inner_factor,) = eliminate(inner, [])
    factor = dot(dot_nt(inner_factor[:, :MODES], inverse), basis)
    for copy in range(out_ref.shape[0]):
        out_ref[copy] = factor


def first_factor(snapshots, sketch_rows, copies):
    return pl.pallas_call(
        leaf_kernel,
        out_shape=jax.ShapeDtypeStruct((copies, MODES, COLS), jnp.float32),
        in_specs=[
            pl.BlockSpec(memory_space=pltpu.HBM),
            pl.BlockSpec(memory_space=pltpu.HBM),
        ],
        out_specs=pl.BlockSpec(memory_space=pltpu.VMEM),
        scratch_shapes=[
            pltpu.VMEM((ROWS, COLS), jnp.float32),
            pltpu.VMEM((MODES, COLS), jnp.float32),
            pltpu.VMEM((COLS, COLS), jnp.float32),
            pltpu.SemaphoreType.DMA((STEPS,)),
            pltpu.SemaphoreType.DMA,
        ],
        compiler_params=pltpu.CompilerParams(vmem_limit_bytes=51 * MIB),
        name="leaf_factor",
    )(snapshots, sketch_rows)


def group_kernel(factors_ref, sketch_ref, out_ref):
    half = gram_of_rows(factors_ref[...].reshape(-1, COLS))
    gram = half + half.T
    rough = first_pass(dot(sketch_ref[...], gram))
    inner = dot_nt(dot(rough, gram), rough)
    share = out_ref.shape[0]
    slot = pl.multiple_of(lax.axis_index("grp") * share, share)
    overlap = dot_nt(sketch_ref[pl.ds(slot, share), :], rough)
    inverse, basis = second_pass(rough)
    mixed = dot(dot_nt(overlap, inverse), dot(inverse, inner))
    out_ref[...] = dot(dot_nt(mixed, inverse), basis)


def group_sample(factors, sketch_rows):
    share = MODES // factors.shape[0]
    return pl.pallas_call(
        group_kernel,
        out_shape=jax.ShapeDtypeStruct((share, COLS), jnp.float32),
        in_specs=[pl.BlockSpec(memory_space=pltpu.VMEM)] * 2,
        out_specs=pl.BlockSpec(memory_space=pltpu.VMEM),
        compiler_params=pltpu.CompilerParams(vmem_limit_bytes=16 * MIB),
        name="group_sample",
    )(factors, sketch_rows)


def project_kernel(snap_ref, sample_ref, out_ref, snap_vmem, out_vmem, in_sem, out_sem):
    load = chunk_loads(snap_ref, snap_vmem, in_sem)
    _, basis = second_pass(first_pass(sample_ref[...]))
    basis_high, basis_low = split2(basis)
    projector = partial_product(
        jnp.concatenate([basis_low, basis_high, basis_high], axis=0),
        jnp.concatenate([basis_high, basis_low, basis_high], axis=0),
        (((0,), (0,)), ((), ())),
    )
    high, low = split2(projector)
    block = PAIR * ROWS // STEPS

    def store(k):
        rows = pl.ds(pl.multiple_of(k * block, block), block)
        return pltpu.make_async_copy(out_vmem.at[rows], out_ref.at[rows], out_sem.at[k])

    @pl.loop(0, STEPS // PAIR)
    def _(k):
        for part in range(PAIR):
            load(PAIR * k + part).wait()
        rows = pl.ds(pl.multiple_of(k * block, block), block)
        snap_high, snap_low = split2(snap_vmem[rows, :])
        value = jnp.dot(snap_high, high, preferred_element_type=jnp.float32)
        value += jnp.dot(snap_low, high, preferred_element_type=jnp.float32)
        value += jnp.dot(snap_high, low, preferred_element_type=jnp.float32)
        out_vmem[rows, :] = value.astype(jnp.bfloat16)
        store(k).start()

    @pl.loop(0, STEPS // PAIR)
    def _(k):
        store(k).wait()


def project(snapshots, sample):
    return pl.pallas_call(
        project_kernel,
        out_shape=jax.ShapeDtypeStruct((ROWS, COLS), jnp.bfloat16),
        in_specs=[
            pl.BlockSpec(memory_space=pltpu.HBM),
            pl.BlockSpec(memory_space=pltpu.VMEM),
        ],
        out_specs=pl.BlockSpec(memory_space=pltpu.HBM),
        scratch_shapes=[
            pltpu.VMEM((ROWS, COLS), jnp.float32),
            pltpu.VMEM((ROWS, COLS), jnp.bfloat16),
            pltpu.SemaphoreType.DMA((STEPS,)),
            pltpu.SemaphoreType.DMA((STEPS // PAIR,)),
        ],
        compiler_params=pltpu.CompilerParams(vmem_limit_bytes=51 * MIB),
        name="project",
    )(snapshots, sample)


def to_all(copies, axis, groups=None):
    return lax.all_to_all(
        copies, axis, split_axis=0, concat_axis=0, tiled=True, axis_index_groups=groups
    )


def copied(array, count):
    return jnp.broadcast_to(array, (count, *array.shape))


def local(snapshots, sketch):
    sketch_rows = sketch.T
    members, leaves = lax.axis_size("grp"), lax.axis_size("leaf")
    factors = to_all(first_factor(snapshots, sketch_rows, members), "grp")
    mine = group_sample(factors, sketch_rows)
    mine = mine + lax.ppermute(mine, "leaf", [(i, i ^ 1) for i in range(leaves)])
    chips = [list(range(core, leaves, 2)) for core in range(2)]
    summed = jnp.sum(to_all(copied(mine, leaves // 2), "leaf", chips), axis=0)
    total = to_all(copied(summed, members), "grp").reshape(MODES, COLS)
    return project(snapshots, total)


def solution(mesh):
    return jax.shard_map(
        local,
        mesh=mesh,
        in_specs=(P(("grp", "leaf"), None), P()),
        out_specs=P(("grp", "leaf"), None),
        check_vma=False,
    )
```

```python
import jax
import jax.numpy as jnp
from jax import lax
from jax.experimental import pallas as pl
from jax.experimental.pallas import tpu as pltpu
from jax.sharding import PartitionSpec as P

ROWS = 4096
COLS = 256
MODES = 64
TILE = 8
PANELS = MODES // TILE
LANES = 128
STEPS = 8
PAIR = 2
MIB = 2**20


def product(a, b, dims):
    rows = a.shape[0]
    high, mid, low = split3(a)
    b_high, b_mid, b_low = split3(b)
    by_high = partial_product(jnp.concatenate([high, mid, low], axis=0), b_high, dims)
    by_mid = partial_product(jnp.concatenate([high, mid], axis=0), b_mid, dims)
    by_low = partial_product(high, b_low, dims)
    small = by_low + by_high[2 * rows :] + by_mid[rows:]
    return by_high[:rows] + (by_high[rows : 2 * rows] + by_mid[:rows] + small)


def partial_product(a, b, dims):
    return lax.dot_general(a, b, dims, preferred_element_type=jnp.float32)


def dot(a, b):
    return product(a, b, (((1,), (0,)), ((), ())))


def dot_nt(a, b):
    return product(a, b, (((1,), (1,)), ((), ())))


def gram_of_rows(a):
    high, mid, low = split3(a)
    half = jnp.bfloat16(0.5)
    dims = (((0,), (0,)), ((), ()))
    upper = lax.dot_general(high, high * half, dims, preferred_element_type=jnp.float32)
    upper += lax.dot_general(high, mid, dims, preferred_element_type=jnp.float32)
    upper += lax.dot_general(high, low, dims, preferred_element_type=jnp.float32)
    upper += lax.dot_general(mid, mid * half, dims, preferred_element_type=jnp.float32)
    return upper


def split3(a):
    high = a.astype(jnp.bfloat16)
    rest = a - high.astype(jnp.float32)
    mid = rest.astype(jnp.bfloat16)
    low = (rest - mid.astype(jnp.float32)).astype(jnp.bfloat16)
    return high, mid, low


def split2(a):
    high = a.astype(jnp.bfloat16)
    return high, (a - high.astype(jnp.float32)).astype(jnp.bfloat16)


def lane_splat(tile, lane):
    lanes = lax.broadcasted_iota(jnp.int32, (TILE, LANES), 1)
    one = jnp.sum(jnp.where(lanes == lane, tile, 0.0), axis=1, keepdims=True)
    return jnp.broadcast_to(one, (TILE, LANES))


def row_splat(tile, row):
    return jnp.broadcast_to(tile[row : row + 1, :], tile.shape)


def eliminate(square, others):
    sublane = lax.broadcasted_iota(jnp.int32, (TILE, LANES), 0)
    rows = [
        [m[TILE * i : TILE * (i + 1), :] for m in (square, *others)] for i in range(PANELS)
    ]
    diag = [lane_splat(rows[0][0], j) for j in range(TILE)]
    for t in range(PANELS):
        base = TILE * t
        below = {i: [None] * TILE for i in range(t + 1, PANELS)}
        for j in range(TILE):
            for i in range(t + 1, PANELS):
                below[i][j] = lane_splat(rows[i][0], base + j)
        ahead = (
            [lane_splat(rows[t + 1][0], base + TILE + l) for l in range(TILE)]
            if t + 1 < PANELS
            else None
        )
        pivots = None
        for j in range(TILE):
            pivot = row_splat(diag[j], j)
            inverse = 1.0 / pivot
            pivots = pivot if pivots is None else jnp.where(sublane == j, pivot, pivots)
            pivot_rows = [row_splat(part, j) for part in rows[t]]
            column = {l: row_splat(diag[l], j) for l in range(j + 1, TILE)}
            if j + 1 < TILE:
                factor = jnp.where(sublane > j, diag[j] * inverse, 0.0)
                for l in range(j + 1, TILE):
                    diag[l] = diag[l] - factor * column[l]
                rows[t] = [part - factor * row for part, row in zip(rows[t], pivot_rows)]
            for i in range(t + 1, PANELS):
                factor = below[i][j] * inverse
                if i == t + 1:
                    for l in range(TILE):
                        ahead[l] = ahead[l] - factor * row_splat(below[i][j], l)
                for l in range(j + 1, TILE):
                    below[i][l] = below[i][l] - factor * column[l]
                rows[i] = [part - factor * row for part, row in zip(rows[i], pivot_rows)]
        scale = lax.rsqrt(pivots)
        rows[t] = [part * scale for part in rows[t]]
        diag = ahead
    count = 1 + len(others)
    return [jnp.concatenate([rows[i][k] for i in range(PANELS)], axis=0) for k in range(count)]


def halves(a):
    return [a[:, :LANES], a[:, LANES:]]


def wide(a):
    return jnp.concatenate([a, jnp.zeros_like(a)], axis=0)


def identity_right():
    row = lax.broadcasted_iota(jnp.int32, (MODES, LANES), 0)
    lane = lax.broadcasted_iota(jnp.int32, (MODES, LANES), 1)
    return jnp.where(lane == row + MODES, 1.0, 0.0).astype(jnp.float32)


def first_pass(sample):
    _, *parts = eliminate(dot_nt(sample, wide(sample)), halves(sample))
    return jnp.concatenate(parts, axis=1)


def second_pass(rough):
    square, *parts = eliminate(dot_nt(rough, wide(rough)) + identity_right(), halves(rough))
    return square[:, MODES:], jnp.concatenate(parts, axis=1)


def chunk_loads(snap_ref, snap_vmem, sem):
    block = ROWS // STEPS

    def load(k):
        rows = pl.ds(pl.multiple_of(k * block, block), block)
        return pltpu.make_async_copy(snap_ref.at[rows], snap_vmem.at[rows], sem.at[k])

    for k in range(STEPS):
        load(k).start()
    return load


def orthonormalise(rows_ref):
    @pl.loop(0, 2)
    def _(_):
        rows_ref[...] = first_pass(rows_ref[...])


def gram_kernel(snap_ref, out_ref, snap_vmem, sem):
    load = chunk_loads(snap_ref, snap_vmem, sem)
    block = PAIR * ROWS // STEPS
    out_ref[...] = jnp.zeros_like(out_ref)

    @pl.loop(0, STEPS // PAIR)
    def _(k):
        for part in range(PAIR):
            load(PAIR * k + part).wait()
        out_ref[...] += gram_of_rows(snap_vmem[pl.ds(pl.multiple_of(k * block, block), block), :])


def half_gram(snapshots):
    return pl.pallas_call(
        gram_kernel,
        out_shape=jax.ShapeDtypeStruct((COLS, COLS), jnp.float32),
        in_specs=[pl.BlockSpec(memory_space=pltpu.HBM)],
        out_specs=pl.BlockSpec(memory_space=pltpu.VMEM),
        scratch_shapes=[
            pltpu.VMEM((ROWS, COLS), jnp.float32),
            pltpu.SemaphoreType.DMA((STEPS,)),
        ],
        compiler_params=pltpu.CompilerParams(vmem_limit_bytes=51 * MIB),
        name="half_gram",
    )(snapshots)


def leaf_kernel(gram_ref, sketch_ref, out_ref):
    half = gram_ref[...]
    gram = half + half.T
    rough = first_pass(dot(sketch_ref[...], gram))
    inner = dot_nt(dot(rough, gram), wide(rough))
    inverse, basis = second_pass(rough)
    (inner_factor,) = eliminate(inner, [])
    factor = dot(dot_nt(inner_factor[:, :MODES], inverse), basis)
    for copy in range(out_ref.shape[0]):
        out_ref[copy] = factor


def first_factor(half, sketch_rows, copies):
    return pl.pallas_call(
        leaf_kernel,
        out_shape=jax.ShapeDtypeStruct((copies, MODES, COLS), jnp.float32),
        in_specs=[pl.BlockSpec(memory_space=pltpu.VMEM)] * 2,
        out_specs=pl.BlockSpec(memory_space=pltpu.VMEM),
        compiler_params=pltpu.CompilerParams(vmem_limit_bytes=16 * MIB),
        name="leaf_factor",
    )(half, sketch_rows)


def group_kernel(factors_ref, sketch_ref, out_ref, basis_ref, gram_ref):
    half = gram_of_rows(factors_ref[...].reshape(-1, COLS))
    gram_ref[...] = half + half.T
    basis_ref[...] = dot(sketch_ref[...], gram_ref[...])
    orthonormalise(basis_ref)
    basis = basis_ref[...]
    inner = dot_nt(dot(basis, gram_ref[...]), basis)
    share = out_ref.shape[0]
    slot = pl.multiple_of(lax.axis_index("grp") * share, share)
    overlap = dot_nt(sketch_ref[pl.ds(slot, share), :], basis)
    out_ref[...] = dot(dot(overlap, inner), basis)


def group_sample(factors, sketch_rows):
    share = MODES // factors.shape[0]
    return pl.pallas_call(
        group_kernel,
        out_shape=jax.ShapeDtypeStruct((share, COLS), jnp.float32),
        in_specs=[pl.BlockSpec(memory_space=pltpu.VMEM)] * 2,
        out_specs=pl.BlockSpec(memory_space=pltpu.VMEM),
        scratch_shapes=[
            pltpu.VMEM((MODES, COLS), jnp.float32),
            pltpu.VMEM((COLS, COLS), jnp.float32),
        ],
        compiler_params=pltpu.CompilerParams(vmem_limit_bytes=16 * MIB),
        name="group_sample",
    )(factors, sketch_rows)


def project_kernel(
    snap_ref, sample_ref, out_ref, snap_vmem, out_vmem, basis_ref, in_sem, out_sem
):
    load = chunk_loads(snap_ref, snap_vmem, in_sem)
    basis_ref[...] = sample_ref[...]
    orthonormalise(basis_ref)
    basis_high, basis_low = split2(basis_ref[...])
    projector = partial_product(
        jnp.concatenate([basis_low, basis_high, basis_high], axis=0),
        jnp.concatenate([basis_high, basis_low, basis_high], axis=0),
        (((0,), (0,)), ((), ())),
    )
    high, low = split2(projector)
    block = PAIR * ROWS // STEPS

    def store(k):
        rows = pl.ds(pl.multiple_of(k * block, block), block)
        return pltpu.make_async_copy(out_vmem.at[rows], out_ref.at[rows], out_sem.at[k])

    @pl.loop(0, STEPS // PAIR)
    def _(k):
        for part in range(PAIR):
            load(PAIR * k + part).wait()
        rows = pl.ds(pl.multiple_of(k * block, block), block)
        snap_high, snap_low = split2(snap_vmem[rows, :])
        value = jnp.dot(snap_high, high, preferred_element_type=jnp.float32)
        value += jnp.dot(snap_low, high, preferred_element_type=jnp.float32)
        value += jnp.dot(snap_high, low, preferred_element_type=jnp.float32)
        out_vmem[rows, :] = value.astype(jnp.bfloat16)
        store(k).start()

    @pl.loop(0, STEPS // PAIR)
    def _(k):
        store(k).wait()


def project(snapshots, sample):
    return pl.pallas_call(
        project_kernel,
        out_shape=jax.ShapeDtypeStruct((ROWS, COLS), jnp.bfloat16),
        in_specs=[
            pl.BlockSpec(memory_space=pltpu.HBM),
            pl.BlockSpec(memory_space=pltpu.VMEM),
        ],
        out_specs=pl.BlockSpec(memory_space=pltpu.HBM),
        scratch_shapes=[
            pltpu.VMEM((ROWS, COLS), jnp.float32),
            pltpu.VMEM((ROWS, COLS), jnp.bfloat16),
            pltpu.VMEM((MODES, COLS), jnp.float32),
            pltpu.SemaphoreType.DMA((STEPS,)),
            pltpu.SemaphoreType.DMA((STEPS // PAIR,)),
        ],
        compiler_params=pltpu.CompilerParams(vmem_limit_bytes=51 * MIB),
        name="project",
    )(snapshots, sample)


def to_all(copies, axis, groups=None):
    return lax.all_to_all(
        copies, axis, split_axis=0, concat_axis=0, tiled=True, axis_index_groups=groups
    )


def copied(array, count):
    return jnp.broadcast_to(array, (count, *array.shape))


def local(snapshots, sketch):
    sketch_rows = sketch.T
    members, leaves = lax.axis_size("grp"), lax.axis_size("leaf")
    factors = to_all(first_factor(half_gram(snapshots), sketch_rows, members), "grp")
    mine = group_sample(factors, sketch_rows)
    mine = mine + lax.ppermute(mine, "leaf", [(i, i ^ 1) for i in range(leaves)])
    chips = [list(range(core, leaves, 2)) for core in range(2)]
    summed = jnp.sum(to_all(copied(mine, leaves // 2), "leaf", chips), axis=0)
    total = to_all(copied(summed, members), "grp").reshape(MODES, COLS)
    return project(snapshots, total)


def solution(mesh):
    return jax.shard_map(
        local,
        mesh=mesh,
        in_specs=(P(("grp", "leaf"), None), P()),
        out_specs=P(("grp", "leaf"), None),
        check_vma=False,
    )
```

```python
import jax
import jax.numpy as jnp
from jax import lax
from jax.experimental import pallas as pl
from jax.experimental.pallas import tpu as pltpu
from jax.sharding import PartitionSpec as P

ROWS = 4096
COLS = 256
MODES = 64
TILE = 8
PANELS = MODES // TILE
LANES = 128
STEPS = 8
PAIR = 2
MIB = 2**20


def product(a, b, dims):
    rows = a.shape[0]
    high, mid, low = split3(a)
    b_high, b_mid, b_low = split3(b)
    by_high = partial_product(jnp.concatenate([high, mid, low], axis=0), b_high, dims)
    by_mid = partial_product(jnp.concatenate([high, mid], axis=0), b_mid, dims)
    by_low = partial_product(high, b_low, dims)
    small = by_low + by_high[2 * rows :] + by_mid[rows:]
    return by_high[:rows] + (by_high[rows : 2 * rows] + by_mid[:rows] + small)


def partial_product(a, b, dims):
    return lax.dot_general(a, b, dims, preferred_element_type=jnp.float32)


def dot(a, b):
    return product(a, b, (((1,), (0,)), ((), ())))


def dot_nt(a, b):
    return product(a, b, (((1,), (1,)), ((), ())))


def gram_of_rows(a):
    high, mid, low = split3(a)
    half = jnp.bfloat16(0.5)
    dims = (((0,), (0,)), ((), ()))
    upper = lax.dot_general(high, high * half, dims, preferred_element_type=jnp.float32)
    upper += lax.dot_general(high, mid, dims, preferred_element_type=jnp.float32)
    upper += lax.dot_general(high, low, dims, preferred_element_type=jnp.float32)
    upper += lax.dot_general(mid, mid * half, dims, preferred_element_type=jnp.float32)
    return upper


def split3(a):
    high = a.astype(jnp.bfloat16)
    rest = a - high.astype(jnp.float32)
    mid = rest.astype(jnp.bfloat16)
    low = (rest - mid.astype(jnp.float32)).astype(jnp.bfloat16)
    return high, mid, low


def split2(a):
    high = a.astype(jnp.bfloat16)
    return high, (a - high.astype(jnp.float32)).astype(jnp.bfloat16)


def lane_splat(tile, lane):
    lanes = lax.broadcasted_iota(jnp.int32, (TILE, LANES), 1)
    one = jnp.sum(jnp.where(lanes == lane, tile, 0.0), axis=1, keepdims=True)
    return jnp.broadcast_to(one, (TILE, LANES))


def row_splat(tile, row):
    return jnp.broadcast_to(tile[row : row + 1, :], tile.shape)


def eliminate(square, others):
    sublane = lax.broadcasted_iota(jnp.int32, (TILE, LANES), 0)
    rows = [
        [m[TILE * i : TILE * (i + 1), :] for m in (square, *others)] for i in range(PANELS)
    ]
    diag = [lane_splat(rows[0][0], j) for j in range(TILE)]
    for t in range(PANELS):
        base = TILE * t
        below = {i: [None] * TILE for i in range(t + 1, PANELS)}
        for j in range(TILE):
            for i in range(t + 1, PANELS):
                below[i][j] = lane_splat(rows[i][0], base + j)
        ahead = (
            [lane_splat(rows[t + 1][0], base + TILE + l) for l in range(TILE)]
            if t + 1 < PANELS
            else None
        )
        pivots = None
        for j in range(TILE):
            pivot = row_splat(diag[j], j)
            inverse = 1.0 / pivot
            pivots = pivot if pivots is None else jnp.where(sublane == j, pivot, pivots)
            pivot_rows = [row_splat(part, j) for part in rows[t]]
            column = {l: row_splat(diag[l], j) for l in range(j + 1, TILE)}
            if j + 1 < TILE:
                factor = jnp.where(sublane > j, diag[j] * inverse, 0.0)
                for l in range(j + 1, TILE):
                    diag[l] = diag[l] - factor * column[l]
                rows[t] = [part - factor * row for part, row in zip(rows[t], pivot_rows)]
            for i in range(t + 1, PANELS):
                factor = below[i][j] * inverse
                if i == t + 1:
                    for l in range(TILE):
                        ahead[l] = ahead[l] - factor * row_splat(below[i][j], l)
                for l in range(j + 1, TILE):
                    below[i][l] = below[i][l] - factor * column[l]
                rows[i] = [part - factor * row for part, row in zip(rows[i], pivot_rows)]
        scale = lax.rsqrt(pivots)
        rows[t] = [part * scale for part in rows[t]]
        diag = ahead
    count = 1 + len(others)
    return [jnp.concatenate([rows[i][k] for i in range(PANELS)], axis=0) for k in range(count)]


def halves(a):
    return [a[:, :LANES], a[:, LANES:]]


def wide(a):
    return jnp.concatenate([a, jnp.zeros_like(a)], axis=0)


def identity_right():
    row = lax.broadcasted_iota(jnp.int32, (MODES, LANES), 0)
    lane = lax.broadcasted_iota(jnp.int32, (MODES, LANES), 1)
    return jnp.where(lane == row + MODES, 1.0, 0.0).astype(jnp.float32)


def first_pass(sample):
    _, *parts = eliminate(dot_nt(sample, wide(sample)), halves(sample))
    return jnp.concatenate(parts, axis=1)


def second_pass(rough):
    square, *parts = eliminate(dot_nt(rough, wide(rough)) + identity_right(), halves(rough))
    return square[:, MODES:], jnp.concatenate(parts, axis=1)


def chunk_loads(snap_ref, snap_vmem, sem, first=STEPS):
    block = ROWS // STEPS

    def load(k):
        rows = pl.ds(pl.multiple_of(k * block, block), block)
        return pltpu.make_async_copy(snap_ref.at[rows], snap_vmem.at[rows], sem.at[k])

    for k in range(first):
        load(k).start()
    return load


def orthonormalise(rows_ref):
    @pl.loop(0, 2)
    def _(_):
        rows_ref[...] = first_pass(rows_ref[...])


def gram_kernel(snap_ref, out_ref, snap_vmem, sem):
    load = chunk_loads(snap_ref, snap_vmem, sem, 2 * PAIR)
    block = PAIR * ROWS // STEPS
    out_ref[...] = jnp.zeros_like(out_ref)

    @pl.loop(0, STEPS // PAIR)
    def _(k):
        for part in range(PAIR):
            load(PAIR * k + part).wait()

        @pl.when(k < STEPS // PAIR - 2)
        def _():
            for part in range(PAIR):
                load(PAIR * (k + 2) + part).start()

        out_ref[...] += gram_of_rows(snap_vmem[pl.ds(pl.multiple_of(k * block, block), block), :])


def half_gram(snapshots):
    return pl.pallas_call(
        gram_kernel,
        out_shape=jax.ShapeDtypeStruct((COLS, COLS), jnp.float32),
        in_specs=[pl.BlockSpec(memory_space=pltpu.HBM)],
        out_specs=pl.BlockSpec(memory_space=pltpu.VMEM),
        scratch_shapes=[
            pltpu.VMEM((ROWS, COLS), jnp.float32),
            pltpu.SemaphoreType.DMA((STEPS,)),
        ],
        compiler_params=pltpu.CompilerParams(vmem_limit_bytes=51 * MIB),
        name="half_gram",
    )(snapshots)


def leaf_kernel(gram_ref, sketch_ref, out_ref):
    half = gram_ref[...]
    gram = half + half.T
    rough = first_pass(dot(sketch_ref[...], gram))
    inner = dot_nt(dot(rough, gram), wide(rough))
    inverse, basis = second_pass(rough)
    (inner_factor,) = eliminate(inner, [])
    factor = dot(dot_nt(inner_factor[:, :MODES], inverse), basis)
    for copy in range(out_ref.shape[0]):
        out_ref[copy] = factor


def first_factor(half, sketch_rows, copies):
    return pl.pallas_call(
        leaf_kernel,
        out_shape=jax.ShapeDtypeStruct((copies, MODES, COLS), jnp.float32),
        in_specs=[pl.BlockSpec(memory_space=pltpu.VMEM)] * 2,
        out_specs=pl.BlockSpec(memory_space=pltpu.VMEM),
        compiler_params=pltpu.CompilerParams(vmem_limit_bytes=16 * MIB),
        name="leaf_factor",
    )(half, sketch_rows)


def bend(leaf):
    return lax.rem(lax.div(lax.rem(lax.div(leaf, 2), 4) + 1, 2), 2)


def bent(leaf):
    return (leaf // 2 % 4 + 1) // 2 % 2


def share_index():
    half = lax.axis_size("grp") // 2
    member = lax.axis_index("grp")
    return lax.rem(member + half * bend(lax.axis_index("leaf")), 2 * half)


def group_kernel(factors_ref, sketch_ref, out_ref, basis_ref, gram_ref):
    half = gram_of_rows(factors_ref[...].reshape(-1, COLS))
    gram_ref[...] = half + half.T
    basis_ref[...] = dot(sketch_ref[...], gram_ref[...])
    orthonormalise(basis_ref)
    basis = basis_ref[...]
    inner = dot_nt(dot(basis, gram_ref[...]), basis)
    share = out_ref.shape[0]
    slot = pl.multiple_of(share_index() * share, share)
    overlap = dot_nt(sketch_ref[pl.ds(slot, share), :], basis)
    out_ref[...] = dot(dot(overlap, inner), basis)


def group_sample(factors, sketch_rows):
    share = MODES // factors.shape[0]
    return pl.pallas_call(
        group_kernel,
        out_shape=jax.ShapeDtypeStruct((share, COLS), jnp.float32),
        in_specs=[pl.BlockSpec(memory_space=pltpu.VMEM)] * 2,
        out_specs=pl.BlockSpec(memory_space=pltpu.VMEM),
        scratch_shapes=[
            pltpu.VMEM((MODES, COLS), jnp.float32),
            pltpu.VMEM((COLS, COLS), jnp.float32),
        ],
        compiler_params=pltpu.CompilerParams(vmem_limit_bytes=16 * MIB),
        name="group_sample",
    )(factors, sketch_rows)


def project_kernel(
    snap_ref, sample_ref, out_ref, snap_vmem, out_vmem, basis_ref, in_sem, out_sem
):
    load = chunk_loads(snap_ref, snap_vmem, in_sem)
    basis_ref[...] = sample_ref[...]
    orthonormalise(basis_ref)
    basis_high, basis_low = split2(basis_ref[...])
    projector = partial_product(
        jnp.concatenate([basis_low, basis_high, basis_high], axis=0),
        jnp.concatenate([basis_high, basis_low, basis_high], axis=0),
        (((0,), (0,)), ((), ())),
    )
    high, low = split2(projector)
    block = PAIR * ROWS // STEPS

    def store(k):
        rows = pl.ds(pl.multiple_of(k * block, block), block)
        return pltpu.make_async_copy(out_vmem.at[rows], out_ref.at[rows], out_sem.at[k])

    @pl.loop(0, STEPS // PAIR)
    def _(k):
        for part in range(PAIR):
            load(PAIR * k + part).wait()
        rows = pl.ds(pl.multiple_of(k * block, block), block)
        snap_high, snap_low = split2(snap_vmem[rows, :])
        value = jnp.dot(snap_high, high, preferred_element_type=jnp.float32)
        value += jnp.dot(snap_low, high, preferred_element_type=jnp.float32)
        value += jnp.dot(snap_high, low, preferred_element_type=jnp.float32)
        out_vmem[rows, :] = value.astype(jnp.bfloat16)
        store(k).start()

    @pl.loop(0, STEPS // PAIR)
    def _(k):
        store(k).wait()


def project(snapshots, sample):
    return pl.pallas_call(
        project_kernel,
        out_shape=jax.ShapeDtypeStruct((ROWS, COLS), jnp.bfloat16),
        in_specs=[
            pl.BlockSpec(memory_space=pltpu.HBM),
            pl.BlockSpec(memory_space=pltpu.VMEM),
        ],
        out_specs=pl.BlockSpec(memory_space=pltpu.HBM),
        scratch_shapes=[
            pltpu.VMEM((ROWS, COLS), jnp.float32),
            pltpu.VMEM((ROWS, COLS), jnp.bfloat16),
            pltpu.VMEM((MODES, COLS), jnp.float32),
            pltpu.SemaphoreType.DMA((STEPS,)),
            pltpu.SemaphoreType.DMA((STEPS // PAIR,)),
        ],
        compiler_params=pltpu.CompilerParams(vmem_limit_bytes=51 * MIB),
        name="project",
    )(snapshots, sample)


def to_all(copies, axis, groups=None):
    return lax.all_to_all(
        copies, axis, split_axis=0, concat_axis=0, tiled=True, axis_index_groups=groups
    )


def copied(array, count):
    return jnp.broadcast_to(array, (count, *array.shape))


def local(snapshots, sketch):
    sketch_rows = sketch.T
    members, leaves = lax.axis_size("grp"), lax.axis_size("leaf")
    factors = to_all(first_factor(half_gram(snapshots), sketch_rows, members), "grp")
    mine = group_sample(factors, sketch_rows)
    mine = mine + lax.ppermute(mine, "leaf", [(i, i ^ 1) for i in range(leaves)])
    chips = [
        [
            (share + members // 2 * bent(leaf)) % members * leaves + leaf
            for leaf in range(core, leaves, 2)
        ]
        for share in range(members)
        for core in range(2)
    ]
    summed = jnp.sum(to_all(copied(mine, leaves // 2), ("grp", "leaf"), chips), axis=0)
    total = to_all(copied(summed, members), "grp").reshape(MODES, COLS)
    return project(snapshots, total)


def solution(mesh):
    return jax.shard_map(
        local,
        mesh=mesh,
        in_specs=(P(("grp", "leaf"), None), P()),
        out_specs=P(("grp", "leaf"), None),
        check_vma=False,
    )
```

```python
import jax
import jax.numpy as jnp
from jax import lax
from jax.experimental import pallas as pl
from jax.experimental.pallas import tpu as pltpu
from jax.sharding import PartitionSpec as P

ROWS = 4096
COLS = 256
MODES = 64
TILE = 8
PANELS = MODES // TILE
LANES = 128
STEPS = 8
PAIR = 2
MIB = 2**20


def product(a, b, dims):
    rows = a.shape[0]
    high, mid, low = split3(a)
    b_high, b_mid, b_low = split3(b)
    by_high = partial_product(jnp.concatenate([high, mid, low], axis=0), b_high, dims)
    by_mid = partial_product(jnp.concatenate([high, mid], axis=0), b_mid, dims)
    by_low = partial_product(high, b_low, dims)
    small = by_low + by_high[2 * rows :] + by_mid[rows:]
    return by_high[:rows] + (by_high[rows : 2 * rows] + by_mid[:rows] + small)


def partial_product(a, b, dims):
    return lax.dot_general(a, b, dims, preferred_element_type=jnp.float32)


def dot(a, b):
    return product(a, b, (((1,), (0,)), ((), ())))


def dot_nt(a, b):
    return product(a, b, (((1,), (1,)), ((), ())))


def gram_of_rows(a):
    high, mid, low = split3(a)
    half = jnp.bfloat16(0.5)
    dims = (((0,), (0,)), ((), ()))
    upper = lax.dot_general(high, high * half, dims, preferred_element_type=jnp.float32)
    upper += lax.dot_general(high, mid, dims, preferred_element_type=jnp.float32)
    upper += lax.dot_general(mid, mid * half, dims, preferred_element_type=jnp.float32)
    return upper


def split3(a):
    high = a.astype(jnp.bfloat16)
    rest = a - high.astype(jnp.float32)
    mid = rest.astype(jnp.bfloat16)
    low = (rest - mid.astype(jnp.float32)).astype(jnp.bfloat16)
    return high, mid, low


def split2(a):
    high = a.astype(jnp.bfloat16)
    return high, (a - high.astype(jnp.float32)).astype(jnp.bfloat16)


def lane_splat(tile, lane):
    lanes = lax.broadcasted_iota(jnp.int32, (TILE, LANES), 1)
    one = jnp.sum(jnp.where(lanes == lane, tile, 0.0), axis=1, keepdims=True)
    return jnp.broadcast_to(one, (TILE, LANES))


def row_splat(tile, row):
    return jnp.broadcast_to(tile[row : row + 1, :], tile.shape)


def eliminate(square, others):
    sublane = lax.broadcasted_iota(jnp.int32, (TILE, LANES), 0)
    rows = [
        [m[TILE * i : TILE * (i + 1), :] for m in (square, *others)] for i in range(PANELS)
    ]
    diag = [lane_splat(rows[0][0], j) for j in range(TILE)]
    for t in range(PANELS):
        base = TILE * t
        below = {i: [None] * TILE for i in range(t + 1, PANELS)}
        for j in range(TILE):
            for i in range(t + 1, PANELS):
                below[i][j] = lane_splat(rows[i][0], base + j)
        ahead = (
            [lane_splat(rows[t + 1][0], base + TILE + l) for l in range(TILE)]
            if t + 1 < PANELS
            else None
        )
        pivots = None
        for j in range(TILE):
            pivot = row_splat(diag[j], j)
            inverse = 1.0 / pivot
            pivots = pivot if pivots is None else jnp.where(sublane == j, pivot, pivots)
            pivot_rows = [row_splat(part, j) for part in rows[t]]
            column = {l: row_splat(diag[l], j) for l in range(j + 1, TILE)}
            if j + 1 < TILE:
                factor = jnp.where(sublane > j, diag[j] * inverse, 0.0)
                for l in range(j + 1, TILE):
                    diag[l] = diag[l] - factor * column[l]
                rows[t] = [part - factor * row for part, row in zip(rows[t], pivot_rows)]
            for i in range(t + 1, PANELS):
                factor = below[i][j] * inverse
                if i == t + 1:
                    for l in range(TILE):
                        ahead[l] = ahead[l] - factor * row_splat(below[i][j], l)
                for l in range(j + 1, TILE):
                    below[i][l] = below[i][l] - factor * column[l]
                rows[i] = [part - factor * row for part, row in zip(rows[i], pivot_rows)]
        scale = lax.rsqrt(pivots)
        rows[t] = [part * scale for part in rows[t]]
        diag = ahead
    count = 1 + len(others)
    return [jnp.concatenate([rows[i][k] for i in range(PANELS)], axis=0) for k in range(count)]


def halves(a):
    return [a[:, :LANES], a[:, LANES:]]


def wide(a):
    return jnp.concatenate([a, jnp.zeros_like(a)], axis=0)


def identity_right():
    row = lax.broadcasted_iota(jnp.int32, (MODES, LANES), 0)
    lane = lax.broadcasted_iota(jnp.int32, (MODES, LANES), 1)
    return jnp.where(lane == row + MODES, 1.0, 0.0).astype(jnp.float32)


def first_pass(sample):
    _, *parts = eliminate(dot_nt(sample, wide(sample)), halves(sample))
    return jnp.concatenate(parts, axis=1)


def second_pass(rough):
    square, *parts = eliminate(dot_nt(rough, wide(rough)) + identity_right(), halves(rough))
    return square[:, MODES:], jnp.concatenate(parts, axis=1)


def chunk_loads(snap_ref, snap_vmem, sem, first=STEPS):
    block = ROWS // STEPS

    def load(k):
        rows = pl.ds(pl.multiple_of(k * block, block), block)
        return pltpu.make_async_copy(snap_ref.at[rows], snap_vmem.at[rows], sem.at[k])

    for k in range(first):
        load(k).start()
    return load


def orthonormalise(rows_ref):
    @pl.loop(0, 2)
    def _(_):
        rows_ref[...] = first_pass(rows_ref[...])


def gram_kernel(snap_ref, out_ref, snap_vmem, sem):
    load = chunk_loads(snap_ref, snap_vmem, sem, 2 * PAIR)
    block = PAIR * ROWS // STEPS
    out_ref[...] = jnp.zeros_like(out_ref)

    @pl.loop(0, STEPS // PAIR)
    def _(k):
        for part in range(PAIR):
            load(PAIR * k + part).wait()

        @pl.when(k < STEPS // PAIR - 2)
        def _():
            for part in range(PAIR):
                load(PAIR * (k + 2) + part).start()

        out_ref[...] += gram_of_rows(snap_vmem[pl.ds(pl.multiple_of(k * block, block), block), :])


def half_gram(snapshots):
    return pl.pallas_call(
        gram_kernel,
        out_shape=jax.ShapeDtypeStruct((COLS, COLS), jnp.float32),
        in_specs=[pl.BlockSpec(memory_space=pltpu.HBM)],
        out_specs=pl.BlockSpec(memory_space=pltpu.VMEM),
        scratch_shapes=[
            pltpu.VMEM((ROWS, COLS), jnp.float32),
            pltpu.SemaphoreType.DMA((STEPS,)),
        ],
        compiler_params=pltpu.CompilerParams(vmem_limit_bytes=51 * MIB),
        name="half_gram",
    )(snapshots)


def leaf_kernel(gram_ref, sketch_ref, out_ref):
    half = gram_ref[...]
    gram = half + half.T
    rough = first_pass(dot(sketch_ref[...], gram))
    inner = dot_nt(dot(rough, gram), wide(rough))
    inverse, basis = second_pass(rough)
    (inner_factor,) = eliminate(inner, [])
    factor = dot(dot_nt(inner_factor[:, :MODES], inverse), basis)
    for copy in range(out_ref.shape[0]):
        out_ref[copy] = factor


def first_factor(half, sketch_rows, copies):
    return pl.pallas_call(
        leaf_kernel,
        out_shape=jax.ShapeDtypeStruct((copies, MODES, COLS), jnp.float32),
        in_specs=[pl.BlockSpec(memory_space=pltpu.VMEM)] * 2,
        out_specs=pl.BlockSpec(memory_space=pltpu.VMEM),
        compiler_params=pltpu.CompilerParams(vmem_limit_bytes=16 * MIB),
        name="leaf_factor",
    )(half, sketch_rows)


def group_kernel(factors_ref, sketch_ref, keep_ref, send_ref, basis_ref, gram_ref):
    half = gram_of_rows(factors_ref[...].reshape(-1, COLS))
    gram_ref[...] = half + half.T
    basis_ref[...] = dot(sketch_ref[...], gram_ref[...])
    orthonormalise(basis_ref)
    basis = basis_ref[...]
    inner = dot_nt(dot(basis, gram_ref[...]), basis)
    share = keep_ref.shape[0]
    column = lax.rem(lax.axis_index("grp"), lax.axis_size("grp") // 2)
    slot = pl.multiple_of(column * 2 * share, 2 * share)
    overlap = dot_nt(sketch_ref[pl.ds(slot, 2 * share), :], basis)
    rows = dot(dot(overlap, inner), basis)
    first = lax.rem(lax.axis_index("leaf"), 2) == 0
    keep_ref[...] = jnp.where(first, rows[:share], rows[share:])
    send_ref[...] = jnp.where(first, rows[share:], rows[:share])


def group_sample(factors, sketch_rows):
    share = MODES // factors.shape[0]
    rows = jax.ShapeDtypeStruct((share, COLS), jnp.float32)
    return pl.pallas_call(
        group_kernel,
        out_shape=[rows, rows],
        in_specs=[pl.BlockSpec(memory_space=pltpu.VMEM)] * 2,
        out_specs=[pl.BlockSpec(memory_space=pltpu.VMEM)] * 2,
        scratch_shapes=[
            pltpu.VMEM((MODES, COLS), jnp.float32),
            pltpu.VMEM((COLS, COLS), jnp.float32),
        ],
        compiler_params=pltpu.CompilerParams(vmem_limit_bytes=16 * MIB),
        name="group_sample",
    )(factors, sketch_rows)


def project_kernel(
    snap_ref, sample_ref, out_ref, snap_vmem, out_vmem, basis_ref, in_sem, out_sem
):
    load = chunk_loads(snap_ref, snap_vmem, in_sem)
    basis_ref[...] = sample_ref[...]
    orthonormalise(basis_ref)
    basis_high, basis_low = split2(basis_ref[...])
    projector = partial_product(
        jnp.concatenate([basis_low, basis_high, basis_high], axis=0),
        jnp.concatenate([basis_high, basis_low, basis_high], axis=0),
        (((0,), (0,)), ((), ())),
    )
    high, low = split2(projector)
    block = PAIR * ROWS // STEPS

    def store(k):
        rows = pl.ds(pl.multiple_of(k * block, block), block)
        return pltpu.make_async_copy(out_vmem.at[rows], out_ref.at[rows], out_sem.at[k])

    @pl.loop(0, STEPS // PAIR)
    def _(k):
        for part in range(PAIR):
            load(PAIR * k + part).wait()
        rows = pl.ds(pl.multiple_of(k * block, block), block)
        snap_high, snap_low = split2(snap_vmem[rows, :])
        value = jnp.dot(snap_high, high, preferred_element_type=jnp.float32)
        value += jnp.dot(snap_low, high, preferred_element_type=jnp.float32)
        value += jnp.dot(snap_high, low, preferred_element_type=jnp.float32)
        out_vmem[rows, :] = value.astype(jnp.bfloat16)
        store(k).start()

    @pl.loop(0, STEPS // PAIR)
    def _(k):
        store(k).wait()


def project(snapshots, sample):
    return pl.pallas_call(
        project_kernel,
        out_shape=jax.ShapeDtypeStruct((ROWS, COLS), jnp.bfloat16),
        in_specs=[
            pl.BlockSpec(memory_space=pltpu.HBM),
            pl.BlockSpec(memory_space=pltpu.VMEM),
        ],
        out_specs=pl.BlockSpec(memory_space=pltpu.HBM),
        scratch_shapes=[
            pltpu.VMEM((ROWS, COLS), jnp.float32),
            pltpu.VMEM((ROWS, COLS), jnp.bfloat16),
            pltpu.VMEM((MODES, COLS), jnp.float32),
            pltpu.SemaphoreType.DMA((STEPS,)),
            pltpu.SemaphoreType.DMA((STEPS // PAIR,)),
        ],
        compiler_params=pltpu.CompilerParams(vmem_limit_bytes=51 * MIB),
        name="project",
    )(snapshots, sample)


def to_all(copies, axis, groups=None):
    return lax.all_to_all(
        copies, axis, split_axis=0, concat_axis=0, tiled=True, axis_index_groups=groups
    )


def copied(array, count):
    return jnp.broadcast_to(array, (count, *array.shape))


def local(snapshots, sketch):
    sketch_rows = sketch.T
    members, leaves = lax.axis_size("grp"), lax.axis_size("leaf")
    factors = to_all(first_factor(half_gram(snapshots), sketch_rows, members), "grp")
    keep, send = group_sample(factors, sketch_rows)
    mine = keep + lax.ppermute(send, "leaf", [(i, i ^ 1) for i in range(leaves)])
    columns = members // 2

    def device(half, column, leaf):
        return (half * columns + column) * leaves + leaf

    adders = [
        [
            device(half ^ ((leaf // 2 % 4 + 1) // 2 % 2), column, leaf)
            for leaf in range(core, leaves, 2)
        ]
        for half in range(2)
        for column in range(columns)
        for core in range(2)
    ]
    sharers = [
        [device(half, column, leaf + core) for column in range(columns) for core in range(2)]
        for half in range(2)
        for leaf in range(0, leaves, 2)
    ]
    summed = jnp.sum(to_all(copied(mine, leaves // 2), ("grp", "leaf"), adders), axis=0)
    total = to_all(copied(summed, members), ("grp", "leaf"), sharers).reshape(MODES, COLS)
    return project(snapshots, total)


def solution(mesh):
    return jax.shard_map(
        local,
        mesh=mesh,
        in_specs=(P(("grp", "leaf"), None), P()),
        out_specs=P(("grp", "leaf"), None),
        check_vma=False,
    )
```

```python
import jax
import jax.numpy as jnp
from jax import lax
from jax.experimental import pallas as pl
from jax.experimental.pallas import tpu as pltpu
from jax.sharding import PartitionSpec as P

ROWS = 4096
COLS = 256
MODES = 64
TILE = 8
PANELS = MODES // TILE
LANES = 128
STEPS = 8
PAIR = 2
MIB = 2**20


def product(a, b, dims):
    rows = a.shape[0]
    high, mid, low = split3(a)
    b_high, b_mid, b_low = split3(b)
    by_high = partial_product(jnp.concatenate([high, mid, low], axis=0), b_high, dims)
    by_mid = partial_product(jnp.concatenate([high, mid], axis=0), b_mid, dims)
    by_low = partial_product(high, b_low, dims)
    small = by_low + by_high[2 * rows :] + by_mid[rows:]
    return by_high[:rows] + (by_high[rows : 2 * rows] + by_mid[:rows] + small)


def partial_product(a, b, dims):
    return lax.dot_general(a, b, dims, preferred_element_type=jnp.float32)


def dot(a, b):
    return product(a, b, (((1,), (0,)), ((), ())))


def dot_nt(a, b):
    return product(a, b, (((1,), (1,)), ((), ())))


def gram_of_rows(a):
    high, mid, low = split3(a)
    half = jnp.bfloat16(0.5)
    dims = (((0,), (0,)), ((), ()))
    upper = lax.dot_general(high, high * half, dims, preferred_element_type=jnp.float32)
    upper += lax.dot_general(high, mid, dims, preferred_element_type=jnp.float32)
    upper += lax.dot_general(mid, mid * half, dims, preferred_element_type=jnp.float32)
    return upper


def split3(a):
    high = a.astype(jnp.bfloat16)
    rest = a - high.astype(jnp.float32)
    mid = rest.astype(jnp.bfloat16)
    low = (rest - mid.astype(jnp.float32)).astype(jnp.bfloat16)
    return high, mid, low


def split2(a):
    high = a.astype(jnp.bfloat16)
    return high, (a - high.astype(jnp.float32)).astype(jnp.bfloat16)


def lane_splat(tile, lane):
    lanes = lax.broadcasted_iota(jnp.int32, (TILE, LANES), 1)
    one = jnp.sum(jnp.where(lanes == lane, tile, 0.0), axis=1, keepdims=True)
    return jnp.broadcast_to(one, (TILE, LANES))


def row_splat(tile, row):
    return jnp.broadcast_to(tile[row : row + 1, :], tile.shape)


def eliminate(square, others):
    sublane = lax.broadcasted_iota(jnp.int32, (TILE, LANES), 0)
    rows = [
        [m[TILE * i : TILE * (i + 1), :] for m in (square, *others)] for i in range(PANELS)
    ]
    diag = [lane_splat(rows[0][0], j) for j in range(TILE)]
    for t in range(PANELS):
        base = TILE * t
        below = {i: [None] * TILE for i in range(t + 1, PANELS)}
        for j in range(TILE):
            for i in range(t + 1, PANELS):
                below[i][j] = lane_splat(rows[i][0], base + j)
        ahead = (
            [lane_splat(rows[t + 1][0], base + TILE + l) for l in range(TILE)]
            if t + 1 < PANELS
            else None
        )
        pivots = None
        for j in range(TILE):
            pivot = row_splat(diag[j], j)
            inverse = 1.0 / pivot
            pivots = pivot if pivots is None else jnp.where(sublane == j, pivot, pivots)
            pivot_rows = [row_splat(part, j) for part in rows[t]]
            column = {l: row_splat(diag[l], j) for l in range(j + 1, TILE)}
            if j + 1 < TILE:
                factor = jnp.where(sublane > j, diag[j] * inverse, 0.0)
                for l in range(j + 1, TILE):
                    diag[l] = diag[l] - factor * column[l]
                rows[t] = [part - factor * row for part, row in zip(rows[t], pivot_rows)]
            for i in range(t + 1, PANELS):
                factor = below[i][j] * inverse
                if i == t + 1:
                    for l in range(TILE):
                        ahead[l] = ahead[l] - factor * row_splat(below[i][j], l)
                for l in range(j + 1, TILE):
                    below[i][l] = below[i][l] - factor * column[l]
                rows[i] = [part - factor * row for part, row in zip(rows[i], pivot_rows)]
        scale = lax.rsqrt(pivots)
        rows[t] = [part * scale for part in rows[t]]
        diag = ahead
    count = 1 + len(others)
    return [jnp.concatenate([rows[i][k] for i in range(PANELS)], axis=0) for k in range(count)]


def halves(a):
    return [a[:, :LANES], a[:, LANES:]]


def wide(a):
    return jnp.concatenate([a, jnp.zeros_like(a)], axis=0)


def identity_right():
    row = lax.broadcasted_iota(jnp.int32, (MODES, LANES), 0)
    lane = lax.broadcasted_iota(jnp.int32, (MODES, LANES), 1)
    return jnp.where(lane == row + MODES, 1.0, 0.0).astype(jnp.float32)


def first_pass(sample):
    _, *parts = eliminate(dot_nt(sample, wide(sample)), halves(sample))
    return jnp.concatenate(parts, axis=1)


def second_pass(rough):
    square, *parts = eliminate(dot_nt(rough, wide(rough)) + identity_right(), halves(rough))
    return square[:, MODES:], jnp.concatenate(parts, axis=1)


def chunk_loads(snap_ref, snap_vmem, sem, first=STEPS):
    block = ROWS // STEPS

    def load(k):
        rows = pl.ds(pl.multiple_of(k * block, block), block)
        return pltpu.make_async_copy(snap_ref.at[rows], snap_vmem.at[rows], sem.at[k])

    for k in range(first):
        load(k).start()
    return load


def orthonormalise(rows_ref):
    @pl.loop(0, 2)
    def _(_):
        rows_ref[...] = first_pass(rows_ref[...])


def gram_kernel(snap_ref, out_ref, snap_vmem, sem):
    load = chunk_loads(snap_ref, snap_vmem, sem, 2 * PAIR)
    block = PAIR * ROWS // STEPS
    out_ref[...] = jnp.zeros_like(out_ref)

    @pl.loop(0, STEPS // PAIR)
    def _(k):
        for part in range(PAIR):
            load(PAIR * k + part).wait()

        @pl.when(k < STEPS // PAIR - 2)
        def _():
            for part in range(PAIR):
                load(PAIR * (k + 2) + part).start()

        out_ref[...] += gram_of_rows(snap_vmem[pl.ds(pl.multiple_of(k * block, block), block), :])


def half_gram(snapshots):
    return pl.pallas_call(
        gram_kernel,
        out_shape=jax.ShapeDtypeStruct((COLS, COLS), jnp.float32),
        in_specs=[pl.BlockSpec(memory_space=pltpu.HBM)],
        out_specs=pl.BlockSpec(memory_space=pltpu.VMEM),
        scratch_shapes=[
            pltpu.VMEM((ROWS, COLS), jnp.float32),
            pltpu.SemaphoreType.DMA((STEPS,)),
        ],
        compiler_params=pltpu.CompilerParams(vmem_limit_bytes=51 * MIB),
        name="half_gram",
    )(snapshots)


def leaf_kernel(gram_ref, sketch_ref, out_ref):
    half = gram_ref[...]
    gram = half + half.T
    rough = first_pass(dot(sketch_ref[...], gram))
    inner = dot_nt(dot(rough, gram), wide(rough))
    inverse, basis = second_pass(rough)
    (inner_factor,) = eliminate(inner, [])
    factor = dot(dot_nt(inner_factor[:, :MODES], inverse), basis)
    for copy in range(out_ref.shape[0]):
        out_ref[copy] = factor


def first_factor(half, sketch_rows, copies):
    return pl.pallas_call(
        leaf_kernel,
        out_shape=jax.ShapeDtypeStruct((copies, MODES, COLS), jnp.float32),
        in_specs=[pl.BlockSpec(memory_space=pltpu.VMEM)] * 2,
        out_specs=pl.BlockSpec(memory_space=pltpu.VMEM),
        compiler_params=pltpu.CompilerParams(vmem_limit_bytes=16 * MIB),
        name="leaf_factor",
    )(half, sketch_rows)


def bend(leaf):
    return lax.rem(lax.div(lax.rem(lax.div(leaf, 2), 4) + 1, 2), 2)


def bent(leaf):
    return (leaf // 2 % 4 + 1) // 2 % 2


def share_index():
    half = lax.axis_size("grp") // 2
    member = lax.axis_index("grp")
    return lax.rem(member + half * bend(lax.axis_index("leaf")), 2 * half)


def group_kernel(factors_ref, sketch_ref, out_ref, basis_ref, gram_ref):
    half = gram_of_rows(factors_ref[...].reshape(-1, COLS))
    gram_ref[...] = half + half.T
    basis_ref[...] = dot(sketch_ref[...], gram_ref[...])
    orthonormalise(basis_ref)
    basis = basis_ref[...]
    inner = dot_nt(dot(basis, gram_ref[...]), basis)
    share = out_ref.shape[0]
    slot = pl.multiple_of(share_index() * share, share)
    overlap = dot_nt(sketch_ref[pl.ds(slot, share), :], basis)
    out_ref[...] = dot(dot(overlap, inner), basis)


def group_sample(factors, sketch_rows):
    share = MODES // factors.shape[0]
    return pl.pallas_call(
        group_kernel,
        out_shape=jax.ShapeDtypeStruct((share, COLS), jnp.float32),
        in_specs=[pl.BlockSpec(memory_space=pltpu.VMEM)] * 2,
        out_specs=pl.BlockSpec(memory_space=pltpu.VMEM),
        scratch_shapes=[
            pltpu.VMEM((MODES, COLS), jnp.float32),
            pltpu.VMEM((COLS, COLS), jnp.float32),
        ],
        compiler_params=pltpu.CompilerParams(vmem_limit_bytes=16 * MIB),
        name="group_sample",
    )(factors, sketch_rows)


def project_kernel(
    snap_ref, sample_ref, out_ref, snap_vmem, out_vmem, basis_ref, in_sem, out_sem
):
    load = chunk_loads(snap_ref, snap_vmem, in_sem)
    basis_ref[...] = sample_ref[...]
    orthonormalise(basis_ref)
    basis_high, basis_low = split2(basis_ref[...])
    projector = partial_product(
        jnp.concatenate([basis_low, basis_high, basis_high], axis=0),
        jnp.concatenate([basis_high, basis_low, basis_high], axis=0),
        (((0,), (0,)), ((), ())),
    )
    high, low = split2(projector)
    block = PAIR * ROWS // STEPS

    def store(k):
        rows = pl.ds(pl.multiple_of(k * block, block), block)
        return pltpu.make_async_copy(out_vmem.at[rows], out_ref.at[rows], out_sem.at[k])

    @pl.loop(0, STEPS // PAIR)
    def _(k):
        for part in range(PAIR):
            load(PAIR * k + part).wait()
        rows = pl.ds(pl.multiple_of(k * block, block), block)
        snap_high, snap_low = split2(snap_vmem[rows, :])
        value = jnp.dot(snap_high, high, preferred_element_type=jnp.float32)
        value += jnp.dot(snap_low, high, preferred_element_type=jnp.float32)
        value += jnp.dot(snap_high, low, preferred_element_type=jnp.float32)
        out_vmem[rows, :] = value.astype(jnp.bfloat16)
        store(k).start()

    @pl.loop(0, STEPS // PAIR)
    def _(k):
        store(k).wait()


def project(snapshots, sample):
    return pl.pallas_call(
        project_kernel,
        out_shape=jax.ShapeDtypeStruct((ROWS, COLS), jnp.bfloat16),
        in_specs=[
            pl.BlockSpec(memory_space=pltpu.HBM),
            pl.BlockSpec(memory_space=pltpu.VMEM),
        ],
        out_specs=pl.BlockSpec(memory_space=pltpu.HBM),
        scratch_shapes=[
            pltpu.VMEM((ROWS, COLS), jnp.float32),
            pltpu.VMEM((ROWS, COLS), jnp.bfloat16),
            pltpu.VMEM((MODES, COLS), jnp.float32),
            pltpu.SemaphoreType.DMA((STEPS,)),
            pltpu.SemaphoreType.DMA((STEPS // PAIR,)),
        ],
        compiler_params=pltpu.CompilerParams(vmem_limit_bytes=51 * MIB),
        name="project",
    )(snapshots, sample)


def to_all(copies, axis, groups=None):
    return lax.all_to_all(
        copies, axis, split_axis=0, concat_axis=0, tiled=True, axis_index_groups=groups
    )


def copied(array, count):
    return jnp.broadcast_to(array, (count, *array.shape))


def local(snapshots, sketch):
    sketch_rows = sketch.T
    members, leaves = lax.axis_size("grp"), lax.axis_size("leaf")
    factors = to_all(first_factor(half_gram(snapshots), sketch_rows, members), "grp")
    mine = group_sample(factors, sketch_rows)
    mine = mine + lax.ppermute(mine, "leaf", [(i, i ^ 1) for i in range(leaves)])
    chips = [
        [
            (share + members // 2 * bent(leaf)) % members * leaves + leaf
            for leaf in range(core, leaves, 2)
        ]
        for share in range(members)
        for core in range(2)
    ]
    summed = jnp.sum(to_all(copied(mine, leaves // 2), ("grp", "leaf"), chips), axis=0)
    total = to_all(copied(summed, members), "grp").reshape(MODES, COLS)
    return project(snapshots, total)


def solution(mesh):
    return jax.shard_map(
        local,
        mesh=mesh,
        in_specs=(P(("grp", "leaf"), None), P()),
        out_specs=P(("grp", "leaf"), None),
        check_vma=False,
    )
```
